32 devices in a mesh: task: 4 (over z), tile: 8 (over y, x, core).
Axes of the slice: x: 2, y: 2, z: 4, core: 2. Of those that a mesh axis runs over, the one named last changes fastest.
Arguments:
- adjusted: bfloat16 [8, 3584, 18944], P('task', 'tile'), may hold values from -6 to 6
- fisher: bfloat16 [8, 3584, 18944], P('task', 'tile'), may hold values from 0.0099487305 to 10
Outputs:
- merged: bfloat16 [3584, 18944], P(None, ('task', 'tile'))
The draws below stay inside these ranges and needn't reach their ends.
All inputs are finite; a program needn't handle non-finite values.
Results may differ from the reference program's by a relative error of at most 0.001.
Values may be sent and summed in bfloat16 or wider, within the bound.
A program may use at most 256 MiB of HBM per device.

```python
import math
import jax
import jax.numpy as jnp
from jax import lax

D = 3584
FF = 18944
MODELS = 8


def level_of(own_key, extent, cuts, least, top_value):
    def one(position, shards_of):
        steps = jax.random.uniform(jax.random.fold_in(jax.random.fold_in(own_key, 6), position), (shards_of,), jnp.float32, least / len(cuts), top_value / len(cuts))
        return jnp.repeat(jnp.exp(steps), extent[position] // shards_of).reshape((-1,) + (1,) * (len(extent) - position - 1))

    factor_of = one(*cuts[0])
    for cut in cuts[1:]:
        factor_of = factor_of * one(*cut)
    return factor_of


def gaussian(stream_key, dims, width, most, shards=(), dtype=jnp.bfloat16):
    array = width * jax.random.normal(stream_key, dims, jnp.float32)
    if shards:
        array = array * level_of(stream_key, dims, shards, -0.22, 0.18)
    return jnp.clip(array, -most, most).astype(dtype)


def setup_inputs(seed: int = 0) -> dict:
    keys = jax.random.split(jax.random.key(seed), 3)
    adjusted = gaussian(keys[0], (MODELS, D, FF), 1.0, 6.0, ((0, 4), (1, 8)))
    fisher = jnp.clip(jnp.exp(math.log(10.0) - 6.912895 * jax.random.uniform(keys[1], (MODELS, D, FF), jnp.float32) ** level_of(keys[1], (MODELS, D, FF), ((0, 4), (1, 8)), -0.2, 0.2)), 0.0099487305, 10.0).astype(jnp.bfloat16)
    return dict(adjusted=adjusted, fisher=fisher)


def reference(adjusted, fisher):
    def accumulate(carry, pair):
        numerator, denominator = carry
        weights, curvature = pair
        scaled = curvature.astype(jnp.float32)
        return (numerator + scaled * weights.astype(jnp.float32), denominator + scaled), None

    zeros = jnp.zeros((D, FF), jnp.float32)
    (numerator, denominator), unused = lax.scan(accumulate, (zeros, zeros), (adjusted, fisher))
    return (numerator / denominator).astype(jnp.bfloat16)
```

```python
import functools
import math
import jax
import jax.numpy as jnp
from jax import lax
from jax.experimental import pallas as pl
from jax.experimental.pallas import tpu as pltpu
from jax.sharding import PartitionSpec as P

MESH = pl.DeviceIdType.MESH
LANES = 128
LOW, HIGH = 0.0099487305, 10.0
ODD, POWER = 15, 24
LIFT = 2.0**8.25
TINY = 2.0**-126
SLOTS = 4
SKEW = 2
LAG = 16
WIDE = 4


def over(width, step, carry):
    big = WIDE * LANES
    trips = width // big
    carry = lax.fori_loop(0, trips, lambda i, v: step(pl.multiple_of(i * big, big), big, v), carry)
    if width % big:
        carry = step(trips * big, width % big, carry)
    return carry


def spread(block, size):
    return jnp.concatenate([block] * (size // LANES), axis=1) if size > LANES else block


def kernel(n, tiles, rows, width, share, adj, fis, out, inbox, loc_a, loc_f, wire, stage, whole,
           loc_sem, send_sem, recv_sem, near_sem, far_sem, own_sem, out_sem):
    me, tile = lax.axis_index("task"), lax.axis_index("tile")
    f32, bf16 = jnp.float32, jnp.bfloat16
    models, height = adj.shape[0], adj.shape[1]
    chunks = height // rows
    half = n // 2
    count = half * chunks
    per_device = models * math.sqrt(LOW * HIGH)
    last = n - 1

    place = (me, last - me)

    def quarter(s, i):
        return half + i // chunks if s == 0 else half - 1 - i // chunks

    def loads(s, i):
        c, slot = lax.rem(i, chunks), lax.rem(i, 2)
        where = (slice(None), pl.ds(pl.multiple_of(c * rows, rows), rows),
                 pl.ds(pl.multiple_of(quarter(s, i) * width, LANES), width))
        return (
            pltpu.make_async_copy(adj.at[where], loc_a.at[s, slot], loc_sem.at[s, slot, 0]),
            pltpu.make_async_copy(fis.at[where], loc_f.at[s, slot], loc_sem.at[s, slot, 1]),
        )

    def sending(s, i):
        slot = lax.rem(i, SLOTS)
        return pltpu.make_async_remote_copy(
            src_ref=wire.at[s, slot], dst_ref=inbox.at[s, i], send_sem=send_sem.at[s, slot],
            recv_sem=recv_sem.at[s, i], device_id={"task": me + 1 if s == 0 else me - 1}, device_id_type=MESH)

    def local(s, slot, lo, size):
        num = den = None
        for m in range(models):
            f = loc_f[s, slot, m, :, pl.ds(lo, size)].astype(f32)
            fa = f * loc_a[s, slot, m, :, pl.ds(lo, size)].astype(f32)
            num, den = (fa, f) if m == 0 else (num + fa, den + f)
        return num, den

    def gathered(s, i, slot, lo, size, unit, centre):
        num, den = local(s, slot, lo, size)
        if unit is None:
            return num, den
        y = inbox[s, i, :, pl.ds(lo, size)].astype(f32)
        level = jnp.log2(inbox[s, i, :, pl.ds(width + lo, size)].astype(f32)) * (1.0 / POWER)
        size_of = jnp.log2(jnp.maximum(jnp.abs(y), TINY)) * (1.0 / ODD - 1.0)
        num = num + (y * jnp.exp2(size_of + level)) * spread(unit * centre, size)
        den = den + jnp.exp2(level) * centre
        return num, den

    def taken(s, i, first):
        if first:
            return None, None, None
        top = inbox[s, i, :, 2 * width:2 * width + LANES].astype(f32)
        return top, top * (1.0 / LIFT), per_device * place[s].astype(f32)

    def encode(s, i, first):
        slot, to = lax.rem(i, 2), lax.rem(i, SLOTS)
        top, unit, centre = taken(s, i, first)

        def peak(lo, size, high):
            for m in range(models):
                a = jnp.abs(loc_a[s, slot, m, :, pl.ds(lo, size)])
                for k in range(size // LANES):
                    high = jnp.maximum(high, a[:, k * LANES:(k + 1) * LANES].astype(f32))
            return high

        start = jnp.full((rows, LANES), 1e-35, f32) if first else top
        high = over(width, peak, start).astype(bf16)
        wire[s, to, :, 2 * width:2 * width + LANES] = high
        factor = LIFT / high.astype(f32)
        shift = -POWER * jnp.log2(per_device * (place[s] + 1).astype(f32))

        def step(lo, size, carry):
            num, den = gathered(s, i, slot, lo, size, unit, centre)
            log = jnp.log2(den)
            x = num * jnp.exp2(-log) * spread(factor, size)
            x2 = x * x
            x3 = x2 * x
            x6 = x3 * x3
            wire[s, to, :, pl.ds(lo, size)] = (x6 * x6 * x3).astype(bf16)
            wire[s, to, :, pl.ds(width + lo, size)] = jnp.exp2(log * POWER + shift).astype(bf16)
            return carry

        over(width, step, 0)

    def finish(s, i):
        slot = lax.rem(i, 2)
        _, unit, centre = taken(s, i, False)

        def step(lo, size, carry):
            num, den = gathered(s, i, slot, lo, size, unit, centre)
            whole[:, pl.ds(lo, size)] = (num / den).astype(bf16)
            return carry

        over(width, step, 0)
        for t in range(tiles):
            stage[i, t] = whole[:, t * share:(t + 1) * share]

    def place_of(i):
        return pl.ds(pl.multiple_of(tile * height + lax.rem(i, chunks) * rows, rows), rows)

    def hand_out(i, to_task, peer, sem):
        return pltpu.make_async_remote_copy(
            src_ref=stage.at[i, peer], dst_ref=out.at[place_of(i)], send_sem=sem, recv_sem=out_sem,
            device_id={"task": to_task, "tile": peer}, device_id_type=MESH)

    def keep(i):
        return pltpu.make_async_copy(stage.at[i, tile], out.at[place_of(i)], own_sem)

    def send_far(s, i):
        for o in range(tiles):
            hand_out(i, quarter(s, i), lax.rem(tile + o, tiles), far_sem).start()

    def send_near(i):
        keep(i).start()
        for o in range(1, tiles):
            hand_out(i, me, lax.rem(tile + o, tiles), near_sem).start()

    def begin(s, i):
        for copy in loads(s, i):
            copy.start()

    def work(s, i):
        @pl.when(i + 1 < count)
        def _():
            begin(s, i + 1)

        for copy in loads(s, i):
            copy.wait()

        @pl.when(jnp.logical_and(place[s] < last, i >= SLOTS))
        def _():
            sending(s, i).wait_send()

        @pl.when(place[s] == 0)
        def _():
            encode(s, i, True)

        @pl.when(place[s] > 0)
        def _():
            sending(s, i).wait_recv()

            @pl.when(place[s] < last)
            def _():
                encode(s, i, False)

            @pl.when(place[s] == last)
            def _():
                finish(s, i)

                @pl.when(i >= count - chunks)
                def _():
                    send_near(i)

        @pl.when(place[s] < last)
        def _():
            sending(s, i).start()

    far = count - chunks
    lag = min(LAG, far)
    begin_far = count + SKEW * last - far + lag

    for s in range(2):
        begin(s, 0)

    def trip(t, carry):
        for s in range(2):
            i = t - SKEW * place[s]

            @pl.when(jnp.logical_and(i >= 0, i < count))
            def _():
                work(s, i)

            @pl.when(jnp.logical_and(place[s] == last, t >= begin_far))
            def _():
                send_far(s, t - begin_far)
        return carry

    lax.fori_loop(0, count + SKEW * last, trip, 0)

    for s in range(2):
        @pl.when(place[s] == last)
        def _():
            def rest(i, carry):
                send_far(s, i)
                return carry

            lax.fori_loop(far - lag, far, rest, 0)

        @pl.when(place[s] < last)
        def _():
            for i in range(count - SLOTS, count):
                sending(s, i).wait_send()

    at_end = jnp.logical_or(me == 0, me == last)

    @pl.when(at_end)
    def _():
        gone = stage.at[pl.ds(0, far)]
        pltpu.make_async_copy(gone, gone, far_sem).wait()
        gone = stage.at[pl.ds(far, chunks), pl.ds(0, tiles - 1)]
        pltpu.make_async_copy(gone, gone, near_sem).wait()
        gone = stage.at[pl.ds(far, chunks), pl.ds(0, 1)]
        pltpu.make_async_copy(gone, gone, own_sem).wait()
        come = out.at[pl.ds(0, (tiles - 1) * height)]
        pltpu.make_async_copy(come, come, out_sem).wait()

    @pl.when(jnp.logical_not(at_end))
    def _():
        pltpu.make_async_copy(out, out, out_sem).wait()


def body(n, tiles, adjusted, fisher):
    models, height, columns = adjusted.shape
    width = columns // n
    share = width // tiles
    rows = next(r for r in (16, 8, height) if height % r == 0)
    chunks = height // rows
    count = n // 2 * chunks
    bf16 = jnp.bfloat16
    line = 2 * width + LANES
    dma = pltpu.SemaphoreType.DMA
    return pl.pallas_call(
        functools.partial(kernel, n, tiles, rows, width, share),
        out_shape=jax.ShapeDtypeStruct((tiles * height, share), bf16),
        in_specs=[pl.BlockSpec(memory_space=pl.ANY)] * 2,
        out_specs=pl.BlockSpec(memory_space=pl.ANY),
        scratch_shapes=[
            pltpu.VMEM((2, count, rows, line), bf16),
            pltpu.VMEM((2, 2, models, rows, width), bf16),
            pltpu.VMEM((2, 2, models, rows, width), bf16),
            pltpu.VMEM((2, SLOTS, rows, line), bf16),
            pltpu.VMEM((count, tiles, rows, share), bf16),
            pltpu.VMEM((rows, width), bf16),
            dma((2, 2, 2)),
            dma((2, SLOTS)),
            dma((2, count)),
            dma,
            dma,
            dma,
            dma,
        ],
        compiler_params=pltpu.CompilerParams(has_side_effects=True, vmem_limit_bytes=63 * 1024 * 1024),
    )(adjusted, fisher)


def solution(mesh):
    return jax.shard_map(
        functools.partial(body, mesh.shape["task"], mesh.shape["tile"]),
        mesh=mesh,
        in_specs=(P("task", "tile", None), P("task", "tile", None)),
        out_specs=P(None, ("task", "tile")),
        check_vma=False,
    )
```

```python
import functools
import math
import jax
import jax.numpy as jnp
from jax import lax
from jax.experimental import pallas as pl
from jax.experimental.pallas import tpu as pltpu
from jax.sharding import PartitionSpec as P

MESH = pl.DeviceIdType.MESH
LANES, FOLD = 128, 8
LOW, HIGH = 0.0099487305, 10.0
ODD, POWER = 15, 24
LIFT = 2.0**8.25
TINY = 2.0**-126
SLOTS = 2
SKEW = 4
EARLY = 16
WIDE = 4


def over(width, step, carry):
    big = WIDE * LANES
    trips = width // big
    carry = lax.fori_loop(0, trips, lambda i, v: step(pl.multiple_of(i * big, big), big, v), carry)
    if width % big:
        carry = step(trips * big, width % big, carry)
    return carry


def spread(block, rows, size):
    block = jnp.concatenate([block] * (rows // FOLD), axis=0) if rows > FOLD else block
    return jnp.concatenate([block] * (size // LANES), axis=1) if size > LANES else block


def streams(n, tiles, rows, width, adj, fis, inbox, tops, loc_a, loc_f, wire, high_out, loc_sem, send_sem, recv_sem, top_sems, finish, late):
    me = lax.axis_index("task")
    f32, bf16 = jnp.float32, jnp.bfloat16
    models, height = adj.shape[0], adj.shape[1]
    chunks = height // rows
    half, last = n // 2, n - 1
    count = half * chunks
    per_device = models * math.sqrt(LOW * HIGH)
    place = (me, last - me)
    turn = first_row(rows, height)

    def loads(s, i):
        q, slot = i // chunks, lax.rem(i, 2)
        column = half + q if s == 0 else half - 1 - q
        where = (slice(None), pl.ds(turn(lax.rem(i, chunks)), rows), pl.ds(pl.multiple_of(column * width, LANES), width))
        return (
            pltpu.make_async_copy(adj.at[where], loc_a.at[s, slot], loc_sem.at[s, slot, 0]),
            pltpu.make_async_copy(fis.at[where], loc_f.at[s, slot], loc_sem.at[s, slot, 1]),
        )

    def sending(s, i):
        slot, to = lax.rem(i, SLOTS), {"task": me + 1 if s == 0 else me - 1}
        return (
            pltpu.make_async_remote_copy(
                src_ref=high_out.at[s, slot], dst_ref=tops.at[s, i], send_sem=top_sems[0].at[s, slot],
                recv_sem=top_sems[1].at[s, i], device_id=to, device_id_type=MESH),
            pltpu.make_async_remote_copy(
                src_ref=wire.at[s, slot], dst_ref=inbox.at[s, i], send_sem=send_sem.at[s, slot],
                recv_sem=recv_sem.at[s, i], device_id=to, device_id_type=MESH),
        )

    def gathered(s, i, lo, size, unit, centre):
        slot = lax.rem(i, 2)
        num = den = None
        for m in range(models):
            f = loc_f[s, slot, m, :, pl.ds(lo, size)].astype(f32)
            fa = f * loc_a[s, slot, m, :, pl.ds(lo, size)].astype(f32)
            num, den = (fa, f) if m == 0 else (num + fa, den + f)
        if unit is None:
            return num, den
        y = inbox[s, i, :, pl.ds(lo, size)].astype(f32)
        level = jnp.log2(inbox[s, i, :, pl.ds(width + lo, size)].astype(f32)) * (1.0 / POWER)
        part = jnp.log2(jnp.maximum(jnp.abs(y), TINY)) * (1.0 / ODD - 1.0)
        num = num + (y * jnp.exp2(part + level)) * spread(unit * centre, rows, size)
        den = den + jnp.exp2(level) * centre
        return num, den

    def taken(s, i):
        top = tops[s, i].astype(f32)
        return top, top * (1.0 / LIFT), per_device * place[s].astype(f32)

    def encode(s, i, first):
        slot, to = lax.rem(i, 2), lax.rem(i, SLOTS)
        top, unit, centre = (jnp.full((FOLD, LANES), 1e-35, f32), None, None) if first else taken(s, i)

        def peak(lo, size, high):
            for m in range(models):
                a = jnp.abs(loc_a[s, slot, m, :, pl.ds(lo, size)].astype(f32))
                for k in range(size // LANES):
                    for h in range(rows // FOLD):
                        high = jnp.maximum(high, a[h * FOLD:(h + 1) * FOLD, k * LANES:(k + 1) * LANES])
            return high

        high = over(width, peak, top).astype(bf16)
        high_out[s, to] = high
        factor = LIFT / high.astype(f32)
        shift = -POWER * jnp.log2(per_device * (place[s] + 1).astype(f32))

        def step(lo, size, carry):
            num, den = gathered(s, i, lo, size, unit, centre)
            log = jnp.log2(den)
            x = num * jnp.exp2(-log) * spread(factor, rows, size)
            x2 = x * x
            x3 = x2 * x
            x6 = x3 * x3
            wire[s, to, :, pl.ds(lo, size)] = (x6 * x6 * x3).astype(bf16)
            wire[s, to, :, pl.ds(width + lo, size)] = jnp.exp2(log * POWER + shift).astype(bf16)
            return carry

        over(width, step, 0)

    def merge(s, i, put):
        _, unit, centre = taken(s, i)

        def step(lo, size, carry):
            num, den = gathered(s, i, lo, size, unit, centre)
            put(lo, size, (num / den).astype(bf16))
            return carry

        over(width, step, 0)

    def begin(s, i):
        for copy in loads(s, i):
            copy.start()

    def ready(s, i):
        @pl.when(i + 1 < count)
        def _():
            begin(s, i + 1)

        for copy in loads(s, i):
            copy.wait()

    def work(s, i):
        fresh = jnp.logical_or(i > 0, place[s] > 0)

        @pl.when(fresh)
        def _():
            ready(s, i)

        @pl.when(jnp.logical_and(place[s] < last, i >= SLOTS))
        def _():
            for copy in sending(s, i):
                copy.wait_send()

        @pl.when(jnp.logical_and(place[s] == 0, fresh))
        def _():
            encode(s, i, True)

        @pl.when(place[s] > 0)
        def _():
            for copy in sending(s, i):
                copy.wait_recv()

            @pl.when(place[s] < last)
            def _():
                encode(s, i, False)

            @pl.when(place[s] == last)
            def _():
                finish(s, i, functools.partial(merge, s, i))

        @pl.when(place[s] < last)
        def _():
            for copy in sending(s, i):
                copy.start()

    barrier = pltpu.get_barrier_semaphore()
    tile = lax.axis_index("tile")

    def greet(d, carry):
        there = {"task": d // tiles, "tile": lax.rem(d, tiles)}

        @pl.when(d != me * tiles + tile)
        def _():
            pl.semaphore_signal(barrier, inc=1, device_id=there, device_id_type=MESH)
        return carry

    lax.fori_loop(0, n * tiles, greet, 0)
    for s in range(2):
        begin(s, 0)

    for s in range(2):
        @pl.when(place[s] == 0)
        def _():
            ready(s, 0)
            encode(s, 0, True)

    pl.semaphore_wait(barrier, n * tiles - 1)

    def trip(t, carry):
        for s in range(2):
            i = t - SKEW * place[s]

            @pl.when(jnp.logical_and(i >= 0, i < count))
            def _():
                work(s, i)

            @pl.when(place[s] == last)
            def _():
                late(s, t)
        return carry

    trips = count + SKEW * last
    lax.fori_loop(0, trips, trip, 0)

    for s in range(2):
        @pl.when(place[s] == last)
        def _():
            late(s, None)

        @pl.when(place[s] < last)
        def _():
            for i in range(count - min(SLOTS, count), count):
                for copy in sending(s, i):
                    copy.wait_send()


def first_row(rows, height):
    if not shared(height):
        return lambda c: pl.multiple_of(c * rows, rows)
    lead = jnp.where(lax.rem(lax.axis_index("tile"), 2) == 0, height - LANES // 2, 0)
    return lambda c: pl.multiple_of(lax.rem(c * rows + lead, height), rows)


def shared(height):
    return height % LANES == LANES // 2


def flipped(n, tiles, rows, width, share, adj, fis, out, inbox, tops, loc_a, loc_f, wire, high_out, stage, group, pair,
            loc_sem, send_sem, recv_sem, top_send, top_recv, pair_sem, near_sem, far_sem, out_sem):
    me, tile = lax.axis_index("task"), lax.axis_index("tile")
    f32, bf16 = jnp.float32, jnp.bfloat16
    height = adj.shape[1]
    chunks, half = height // rows, n // 2
    middle = LANES // 2
    lead, per = middle // rows, LANES // rows
    full = height // LANES
    even = lax.rem(tile, 2) == 0
    first_block = (tile // 2) * (2 * full + 1)
    base = first_block + jnp.where(even, 0, full + 1)
    far = half - 1
    peers = tiles // 2
    first_peer = jnp.where(even, 0, peers)
    mine = (tile >= peers) != even
    strips = pl.cdiv(width // 2, LANES)
    first_strip = jnp.where(even, 0, width // LANES - strips)

    def column(slot):
        block = first_block + full if isinstance(slot, int) else base + slot
        return pl.ds(pl.multiple_of(block * LANES, LANES), LANES)

    def piece(q, slot, peer):
        return stage.at[q, slot, pl.ds(pl.multiple_of(peer * share, 8), share)]

    def handing(s, q, slot, peer, sem):
        return pltpu.make_async_remote_copy(
            src_ref=piece(q, slot, peer), dst_ref=out.at[:, column(slot)], send_sem=sem, recv_sem=out_sem,
            device_id={"task": half + q if s == 0 else half - 1 - q, "tile": peer}, device_id_type=MESH)

    def keep(slot):
        pltpu.make_async_copy(piece(far, slot, tile), out.at[:, column(slot)], out_sem).start()

    def near(s, slot):
        def one(o, carry):
            handing(s, far, slot, lax.rem(tile + o, tiles), near_sem.at[0]).start()
            return carry

        keep(slot)
        lax.fori_loop(1, tiles, one, 0)

    def near_pair(s):
        def one(o, carry):
            handing(s, far, full, first_peer + lax.rem(tile + o, peers), near_sem.at[1]).start()
            return carry

        pl.when(mine)(lambda: keep(full))
        lax.fori_loop(jnp.where(mine, 1, 0), peers, one, 0)

    def turn(q, slot, start, strips, get):
        def step(j, carry):
            at = pl.multiple_of((start + j) * LANES, LANES)
            stage[q, slot, pl.ds(at, LANES), :] = get(at).astype(f32).T.astype(bf16)
            return carry

        lax.fori_loop(0, strips, step, 0)

    def two_halves(q, at):
        own, other = group[pl.ds(LANES, middle), pl.ds(at, LANES)].astype(f32), pair[q, :, pl.ds(at, LANES)].astype(f32)
        return jnp.concatenate([jnp.where(even, own, other), jnp.where(even, other, own)], axis=0)

    def giving(q):
        return pltpu.make_async_remote_copy(
            src_ref=group.at[pl.ds(LANES, middle)], dst_ref=pair.at[q], send_sem=pair_sem.at[0], recv_sem=pair_sem.at[1 + q],
            device_id={"tile": tile + jnp.where(even, 1, -1)}, device_id_type=MESH)

    def finish(s, i, merge):
        q, c = i // chunks, lax.rem(i, chunks)
        at = pl.multiple_of(jnp.where(c < lead, LANES + c * rows, lax.rem(c - lead + per, per) * rows), rows)

        def put(lo, size, value):
            group[pl.ds(at, rows), pl.ds(lo, size)] = value

        merge(put)

        @pl.when(c == lead - 1)
        def _():
            giving(q).start()

        @pl.when(c == 2 * lead - 1)
        def _():
            giving(q).wait()
            turn(q, full, first_strip, strips, functools.partial(two_halves, q))

            @pl.when(q == far)
            def _():
                near_pair(s)

        @pl.when(jnp.logical_and(c >= lead, lax.rem(c - lead + per, per) == per - 1))
        def _():
            slot = (c - lead) // per
            turn(q, slot, 0, width // LANES, lambda at: group[pl.ds(0, LANES), pl.ds(at, LANES)])

            @pl.when(q == far)
            def _():
                near(s, slot)

    trips = half * chunks + SKEW * (n - 1)
    whole_blocks, early = far * full * tiles, min(EARLY, far * full * tiles)

    def far_block(s, p):
        handing(s, p // (full * tiles), lax.rem(p // tiles, full), lax.rem(tile + p, tiles), far_sem.at[0]).start()

    def late(s, t):
        if t is not None:
            @pl.when(t >= trips - early)
            def _():
                far_block(s, t - (trips - early))
            return

        def rest(p, carry):
            far_block(s, p)
            return carry

        lax.fori_loop(early, whole_blocks, rest, 0)

        def last_block(p, carry):
            handing(s, p // peers, full, first_peer + lax.rem(tile + p, peers), far_sem.at[1]).start()
            return carry

        lax.fori_loop(0, far * peers, last_block, 0)

    streams(n, tiles, rows, width, adj, fis, inbox, tops, loc_a, loc_f, wire, high_out, loc_sem, send_sem, recv_sem,
            (top_send, top_recv), finish, late)

    def settle(sem, blocks):
        if blocks:
            gone = out.at[:, pl.ds(0, blocks * LANES)]
            pltpu.make_async_copy(gone, gone, sem).wait()

    @pl.when(jnp.logical_or(me == 0, me == n - 1))
    def _():
        settle(near_sem.at[0], full * (tiles - 1))
        settle(far_sem.at[0], whole_blocks)

        settle(far_sem.at[1], far * peers)
        pl.when(mine)(lambda: settle(near_sem.at[1], peers - 1))
        pl.when(jnp.logical_not(mine))(lambda: settle(near_sem.at[1], peers))

    pltpu.make_async_copy(out, out, out_sem).wait()


def plain(n, tiles, rows, width, share, adj, fis, out, inbox, tops, loc_a, loc_f, wire, high_out, stage, whole,
          loc_sem, send_sem, recv_sem, top_send, top_recv, near_sem, far_sem, out_sem):
    me, tile = lax.axis_index("task"), lax.axis_index("tile")
    height = adj.shape[1]
    chunks, half = height // rows, n // 2
    far = (half - 1) * chunks

    def place_of(i):
        return pl.ds(pl.multiple_of(tile * height + lax.rem(i, chunks) * rows, rows), rows)

    def handing(s, i, peer, sem):
        q = i // chunks
        return pltpu.make_async_remote_copy(
            src_ref=stage.at[i, peer], dst_ref=out.at[place_of(i)], send_sem=sem, recv_sem=out_sem,
            device_id={"task": half + q if s == 0 else half - 1 - q, "tile": peer}, device_id_type=MESH)

    def finish(s, i, merge):
        def put(lo, size, value):
            whole[:, pl.ds(lo, size)] = value

        merge(put)
        for t in range(tiles):
            stage[i, t] = whole[:, t * share:(t + 1) * share]

        @pl.when(i >= far)
        def _():
            pltpu.make_async_copy(stage.at[i, tile], out.at[place_of(i)], out_sem).start()

            def one(o, carry):
                handing(s, i, lax.rem(tile + o, tiles), near_sem).start()
                return carry

            lax.fori_loop(1, tiles, one, 0)

    def late(s, t):
        if t is None:
            def rest(p, carry):
                handing(s, p // tiles, lax.rem(tile + p, tiles), far_sem).start()
                return carry

            lax.fori_loop(0, far * tiles, rest, 0)

    streams(n, tiles, rows, width, adj, fis, inbox, tops, loc_a, loc_f, wire, high_out, loc_sem, send_sem, recv_sem,
            (top_send, top_recv), finish, late)

    @pl.when(jnp.logical_or(me == 0, me == n - 1))
    def _():
        gone = out.at[pl.ds(0, (tiles - 1) * height)]
        pltpu.make_async_copy(gone, gone, near_sem).wait()
        if far:
            gone = stage.at[pl.ds(0, far)]
            pltpu.make_async_copy(gone, gone, far_sem).wait()

    pltpu.make_async_copy(out, out, out_sem).wait()


def body(n, tiles, adjusted, fisher):
    models, height, columns = adjusted.shape
    width = columns // n
    share = width // tiles
    flip = shared(height) and tiles % 2 == 0 and share % 8 == 0
    rows = next(r for r in (16, 8, height) if height % r == 0)
    half, chunks = n // 2, height // rows
    count = half * chunks
    bf16 = jnp.bfloat16
    dma = pltpu.SemaphoreType.DMA
    if flip:
        hold = [
            pltpu.VMEM((half, height // LANES + 1, width, LANES), bf16),
            pltpu.VMEM((LANES + LANES // 2, width), bf16),
            pltpu.VMEM((half, LANES // 2, width), bf16),
        ]
        ends = [dma((1 + half,)), dma((2,)), dma((2,)), dma]
    else:
        hold = [pltpu.VMEM((count, tiles, rows, share), bf16), pltpu.VMEM((rows, width), bf16)]
        ends = [dma, dma, dma]
    out = (share, tiles * height) if flip else (tiles * height, share)
    merged = pl.pallas_call(
        functools.partial(flipped if flip else plain, n, tiles, rows, width, share),
        out_shape=pltpu.VMEM(out, bf16),
        in_specs=[pl.BlockSpec(memory_space=pl.ANY)] * 2,
        out_specs=pl.BlockSpec(memory_space=pl.ANY),
        scratch_shapes=[
            pltpu.VMEM((2, count, rows, 2 * width), bf16),
            pltpu.VMEM((2, count, FOLD, LANES), bf16),
            pltpu.VMEM((2, 2, models, rows, width), bf16),
            pltpu.VMEM((2, 2, models, rows, width), bf16),
            pltpu.VMEM((2, SLOTS, rows, 2 * width), bf16),
            pltpu.VMEM((2, SLOTS, FOLD, LANES), bf16),
            *hold,
            dma((2, 2, 2)),
            dma((2, SLOTS)),
            dma((2, count)),
            dma((2, SLOTS)),
            dma((2, count)),
            *ends,
        ],
        compiler_params=pltpu.CompilerParams(collective_id=0, has_side_effects=True, vmem_limit_bytes=53 * 1024 * 1024),
    )(adjusted, fisher)
    return merged.T if flip else merged


def solution(mesh):
    return jax.shard_map(
        functools.partial(body, mesh.shape["task"], mesh.shape["tile"]),
        mesh=mesh,
        in_specs=(P("task", "tile", None), P("task", "tile", None)),
        out_specs=P(None, ("task", "tile")),
        check_vma=False,
    )
```

```python
import functools
import math
import jax
import jax.numpy as jnp
from jax import lax
from jax.experimental import pallas as pl
from jax.experimental.pallas import tpu as pltpu
from jax.sharding import PartitionSpec as P

MESH = pl.DeviceIdType.MESH
LANES, FOLD = 128, 8
LOW, HIGH = 0.0099487305, 10.0
ODD, POWER = 15, 24
LIFT = 2.0**8.25
TINY = 2.0**-126
SLOTS = 2
SKEW = 4
EARLY = 16
WIDE = 4


def over(width, step, carry):
    big = WIDE * LANES
    trips = width // big
    carry = lax.fori_loop(0, trips, lambda i, v: step(pl.multiple_of(i * big, big), big, v), carry)
    if width % big:
        carry = step(trips * big, width % big, carry)
    return carry


def spread(block, rows, size):
    block = jnp.concatenate([block] * (rows // FOLD), axis=0) if rows > FOLD else block
    return jnp.concatenate([block] * (size // LANES), axis=1) if size > LANES else block


def streams(n, tiles, rows, width, adj, fis, inbox, tops, loc_a, loc_f, wire, high_out, loc_sem, send_sem, recv_sem, top_sems, finish, late):
    me = lax.axis_index("task")
    f32, bf16 = jnp.float32, jnp.bfloat16
    models, height = adj.shape[0], adj.shape[1]
    chunks = height // rows
    half, last = n // 2, n - 1
    count = half * chunks
    per_device = models * math.sqrt(LOW * HIGH)
    place = (me, last - me)
    turn = first_row(rows, height)

    def loads(s, i):
        q, slot = i // chunks, lax.rem(i, 2)
        column = half + q if s == 0 else half - 1 - q
        where = (slice(None), pl.ds(turn(lax.rem(i, chunks)), rows), pl.ds(pl.multiple_of(column * width, LANES), width))
        return (
            pltpu.make_async_copy(adj.at[where], loc_a.at[s, slot], loc_sem.at[s, slot, 0]),
            pltpu.make_async_copy(fis.at[where], loc_f.at[s, slot], loc_sem.at[s, slot, 1]),
        )

    def sending(s, i):
        slot, to = lax.rem(i, SLOTS), {"task": me + 1 if s == 0 else me - 1}
        return (
            pltpu.make_async_remote_copy(
                src_ref=high_out.at[s, slot], dst_ref=tops.at[s, i], send_sem=top_sems[0].at[s, slot],
                recv_sem=top_sems[1].at[s, i], device_id=to, device_id_type=MESH),
            pltpu.make_async_remote_copy(
                src_ref=wire.at[s, slot], dst_ref=inbox.at[s, i], send_sem=send_sem.at[s, slot],
                recv_sem=recv_sem.at[s, i], device_id=to, device_id_type=MESH),
        )

    def gathered(s, i, lo, size, unit, centre):
        slot = lax.rem(i, 2)
        num = den = None
        for m in range(models):
            f = loc_f[s, slot, m, :, pl.ds(lo, size)].astype(f32)
            fa = f * loc_a[s, slot, m, :, pl.ds(lo, size)].astype(f32)
            num, den = (fa, f) if m == 0 else (num + fa, den + f)
        if unit is None:
            return num, den
        y = inbox[s, i, :, pl.ds(lo, size)].astype(f32)
        level = jnp.log2(inbox[s, i, :, pl.ds(width + lo, size)].astype(f32)) * (1.0 / POWER)
        part = jnp.log2(jnp.maximum(jnp.abs(y), TINY)) * (1.0 / ODD - 1.0)
        num = num + (y * jnp.exp2(part + level)) * spread(unit * centre, rows, size)
        den = den + jnp.exp2(level) * centre
        return num, den

    def taken(s, i):
        top = jnp.broadcast_to(tops[s, i], (FOLD, LANES))
        return top, top * (1.0 / LIFT), per_device * place[s].astype(f32)

    def encode(s, i, first):
        slot, to = lax.rem(i, 2), lax.rem(i, SLOTS)
        top, unit, centre = (jnp.full((FOLD, LANES), 1e-35, f32), None, None) if first else taken(s, i)

        def peak(lo, size, high):
            for m in range(models):
                a = jnp.abs(loc_a[s, slot, m, :, pl.ds(lo, size)].astype(f32))
                for k in range(size // LANES):
                    for h in range(rows // FOLD):
                        high = jnp.maximum(high, a[h * FOLD:(h + 1) * FOLD, k * LANES:(k + 1) * LANES])
            return high

        high = jnp.max(over(width, peak, top), axis=0, keepdims=True)
        high_out[s, to] = high
        factor = jnp.broadcast_to(LIFT / high, (FOLD, LANES))
        shift = -POWER * jnp.log2(per_device * (place[s] + 1).astype(f32))

        def step(lo, size, carry):
            num, den = gathered(s, i, lo, size, unit, centre)
            log = jnp.log2(den)
            x = num * jnp.exp2(-log) * spread(factor, rows, size)
            x2 = x * x
            x3 = x2 * x
            x6 = x3 * x3
            wire[s, to, :, pl.ds(lo, size)] = (x6 * x6 * x3).astype(bf16)
            wire[s, to, :, pl.ds(width + lo, size)] = jnp.exp2(log * POWER + shift).astype(bf16)
            return carry

        over(width, step, 0)

    def merge(s, i, put):
        _, unit, centre = taken(s, i)

        def step(lo, size, carry):
            num, den = gathered(s, i, lo, size, unit, centre)
            put(lo, size, (num / den).astype(bf16))
            return carry

        over(width, step, 0)

    def begin(s, i):
        for copy in loads(s, i):
            copy.start()

    def ready(s, i):
        @pl.when(i + 1 < count)
        def _():
            begin(s, i + 1)

        for copy in loads(s, i):
            copy.wait()

    def work(s, i):
        fresh = jnp.logical_or(i > 0, place[s] > 0)

        @pl.when(fresh)
        def _():
            ready(s, i)

        @pl.when(jnp.logical_and(place[s] < last, i >= SLOTS))
        def _():
            for copy in sending(s, i):
                copy.wait_send()

        @pl.when(jnp.logical_and(place[s] == 0, fresh))
        def _():
            encode(s, i, True)

        @pl.when(place[s] > 0)
        def _():
            for copy in sending(s, i):
                copy.wait_recv()

            @pl.when(place[s] < last)
            def _():
                encode(s, i, False)

            @pl.when(place[s] == last)
            def _():
                finish(s, i, functools.partial(merge, s, i))

        @pl.when(place[s] < last)
        def _():
            for copy in sending(s, i):
                copy.start()

    barrier = pltpu.get_barrier_semaphore()
    tile = lax.axis_index("tile")

    first_task = (me // half) * half
    across = jnp.logical_or(me == half - 1, me == half)

    def greet(d, carry):
        there = {"task": first_task + d // tiles, "tile": lax.rem(d, tiles)}

        @pl.when(d != (me - first_task) * tiles + tile)
        def _():
            pl.semaphore_signal(barrier, inc=1, device_id=there, device_id_type=MESH)
        return carry

    for s in range(2):
        begin(s, 0)
    @pl.when(across)
    def _():
        pl.semaphore_signal(
            barrier, inc=1, device_id={"task": jnp.where(me < half, half, half - 1)}, device_id_type=MESH)

    lax.fori_loop(0, half * tiles, greet, 0)

    for s in range(2):
        @pl.when(place[s] == 0)
        def _():
            ready(s, 0)
            encode(s, 0, True)

    pl.semaphore_wait(barrier, half * tiles - 1 + across.astype(jnp.int32))

    def trip(t, carry):
        for s in range(2):
            i = t - SKEW * place[s]

            @pl.when(jnp.logical_and(i >= 0, i < count))
            def _():
                work(s, i)

            @pl.when(place[s] == last)
            def _():
                late(s, t)
        return carry

    trips = count + SKEW * last
    lax.fori_loop(0, trips, trip, 0)

    for s in range(2):
        @pl.when(place[s] == last)
        def _():
            late(s, None)

        @pl.when(place[s] < last)
        def _():
            for i in range(count - min(SLOTS, count), count):
                for copy in sending(s, i):
                    copy.wait_send()


def first_row(rows, height):
    if not shared(height):
        return lambda c: pl.multiple_of(c * rows, rows)
    lead = jnp.where(lax.rem(lax.axis_index("tile"), 2) == 0, height - LANES // 2, 0)
    return lambda c: pl.multiple_of(lax.rem(c * rows + lead, height), rows)


def shared(height):
    return height % LANES == LANES // 2


def flipped(n, tiles, rows, width, share, adj, fis, out, inbox, tops, loc_a, loc_f, wire, high_out, stage, group, pair,
            loc_sem, send_sem, recv_sem, top_send, top_recv, pair_sem, near_sem, far_sem, out_sem):
    me, tile = lax.axis_index("task"), lax.axis_index("tile")
    f32, bf16 = jnp.float32, jnp.bfloat16
    height = adj.shape[1]
    chunks, half = height // rows, n // 2
    middle = LANES // 2
    lead, per = middle // rows, LANES // rows
    full = height // LANES
    even = lax.rem(tile, 2) == 0
    first_block = (tile // 2) * (2 * full + 1)
    base = first_block + jnp.where(even, 0, full + 1)
    far = half - 1
    peers = tiles // 2
    first_peer = jnp.where(even, 0, peers)
    mine = (tile >= peers) != even
    strips = pl.cdiv(width // 2, LANES)
    first_strip = jnp.where(even, 0, width // LANES - strips)

    def column(slot):
        block = first_block + full if isinstance(slot, int) else base + slot
        return pl.ds(pl.multiple_of(block * LANES, LANES), LANES)

    def piece(q, slot, peer):
        return stage.at[q, slot, pl.ds(pl.multiple_of(peer * share, 8), share)]

    def handing(s, q, slot, peer, sem):
        return pltpu.make_async_remote_copy(
            src_ref=piece(q, slot, peer), dst_ref=out.at[:, column(slot)], send_sem=sem, recv_sem=out_sem,
            device_id={"task": half + q if s == 0 else half - 1 - q, "tile": peer}, device_id_type=MESH)

    def keep(slot):
        pltpu.make_async_copy(piece(far, slot, tile), out.at[:, column(slot)], out_sem).start()

    def near(s, slot):
        def one(o, carry):
            handing(s, far, slot, lax.rem(tile + o, tiles), near_sem.at[0]).start()
            return carry

        keep(slot)
        lax.fori_loop(1, tiles, one, 0)

    def near_pair(s):
        def one(o, carry):
            handing(s, far, full, first_peer + lax.rem(tile + o, peers), near_sem.at[1]).start()
            return carry

        pl.when(mine)(lambda: keep(full))
        lax.fori_loop(jnp.where(mine, 1, 0), peers, one, 0)

    def turn(q, slot, start, strips, get):
        def step(j, carry):
            at = pl.multiple_of((start + j) * LANES, LANES)
            stage[q, slot, pl.ds(at, LANES), :] = get(at).astype(f32).T.astype(bf16)
            return carry

        lax.fori_loop(0, strips, step, 0)

    def two_halves(q, at):
        own, other = group[pl.ds(LANES, middle), pl.ds(at, LANES)].astype(f32), pair[q, :, pl.ds(at, LANES)].astype(f32)
        return jnp.concatenate([jnp.where(even, own, other), jnp.where(even, other, own)], axis=0)

    def giving(q):
        return pltpu.make_async_remote_copy(
            src_ref=group.at[pl.ds(LANES, middle)], dst_ref=pair.at[q], send_sem=pair_sem.at[0], recv_sem=pair_sem.at[1 + q],
            device_id={"tile": tile + jnp.where(even, 1, -1)}, device_id_type=MESH)

    def finish(s, i, merge):
        q, c = i // chunks, lax.rem(i, chunks)
        at = pl.multiple_of(jnp.where(c < lead, LANES + c * rows, lax.rem(c - lead + per, per) * rows), rows)

        def put(lo, size, value):
            group[pl.ds(at, rows), pl.ds(lo, size)] = value

        merge(put)

        @pl.when(c == lead - 1)
        def _():
            giving(q).start()

        @pl.when(c == 2 * lead - 1)
        def _():
            giving(q).wait()
            turn(q, full, first_strip, strips, functools.partial(two_halves, q))

            @pl.when(q == far)
            def _():
                near_pair(s)

        @pl.when(jnp.logical_and(c >= lead, lax.rem(c - lead + per, per) == per - 1))
        def _():
            slot = (c - lead) // per
            turn(q, slot, 0, width // LANES, lambda at: group[pl.ds(0, LANES), pl.ds(at, LANES)])

            @pl.when(q == far)
            def _():
                near(s, slot)

    trips = half * chunks + SKEW * (n - 1)
    whole_blocks, early = far * full * tiles, min(EARLY, far * full * tiles)

    def far_block(s, p):
        handing(s, p // (full * tiles), lax.rem(p // tiles, full), lax.rem(tile + p, tiles), far_sem.at[0]).start()

    def late(s, t):
        if t is not None:
            @pl.when(t >= trips - early)
            def _():
                far_block(s, t - (trips - early))
            return

        def rest(p, carry):
            far_block(s, p)
            return carry

        lax.fori_loop(early, whole_blocks, rest, 0)

        def last_block(p, carry):
            handing(s, p // peers, full, first_peer + lax.rem(tile + p, peers), far_sem.at[1]).start()
            return carry

        lax.fori_loop(0, far * peers, last_block, 0)

    streams(n, tiles, rows, width, adj, fis, inbox, tops, loc_a, loc_f, wire, high_out, loc_sem, send_sem, recv_sem,
            (top_send, top_recv), finish, late)

    def settle(sem, blocks):
        if blocks:
            gone = out.at[:, pl.ds(0, blocks * LANES)]
            pltpu.make_async_copy(gone, gone, sem).wait()

    @pl.when(jnp.logical_or(me == 0, me == n - 1))
    def _():
        settle(near_sem.at[0], full * (tiles - 1))
        settle(far_sem.at[0], whole_blocks)

        settle(far_sem.at[1], far * peers)
        pl.when(mine)(lambda: settle(near_sem.at[1], peers - 1))
        pl.when(jnp.logical_not(mine))(lambda: settle(near_sem.at[1], peers))

    pltpu.make_async_copy(out, out, out_sem).wait()


def plain(n, tiles, rows, width, share, adj, fis, out, inbox, tops, loc_a, loc_f, wire, high_out, stage, whole,
          loc_sem, send_sem, recv_sem, top_send, top_recv, near_sem, far_sem, out_sem):
    me, tile = lax.axis_index("task"), lax.axis_index("tile")
    height = adj.shape[1]
    chunks, half = height // rows, n // 2
    far = (half - 1) * chunks

    def place_of(i):
        return pl.ds(pl.multiple_of(tile * height + lax.rem(i, chunks) * rows, rows), rows)

    def handing(s, i, peer, sem):
        q = i // chunks
        return pltpu.make_async_remote_copy(
            src_ref=stage.at[i, peer], dst_ref=out.at[place_of(i)], send_sem=sem, recv_sem=out_sem,
            device_id={"task": half + q if s == 0 else half - 1 - q, "tile": peer}, device_id_type=MESH)

    def finish(s, i, merge):
        def put(lo, size, value):
            whole[:, pl.ds(lo, size)] = value

        merge(put)
        for t in range(tiles):
            stage[i, t] = whole[:, t * share:(t + 1) * share]

        @pl.when(i >= far)
        def _():
            pltpu.make_async_copy(stage.at[i, tile], out.at[place_of(i)], out_sem).start()

            def one(o, carry):
                handing(s, i, lax.rem(tile + o, tiles), near_sem).start()
                return carry

            lax.fori_loop(1, tiles, one, 0)

    def late(s, t):
        if t is None:
            def rest(p, carry):
                handing(s, p // tiles, lax.rem(tile + p, tiles), far_sem).start()
                return carry

            lax.fori_loop(0, far * tiles, rest, 0)

    streams(n, tiles, rows, width, adj, fis, inbox, tops, loc_a, loc_f, wire, high_out, loc_sem, send_sem, recv_sem,
            (top_send, top_recv), finish, late)

    @pl.when(jnp.logical_or(me == 0, me == n - 1))
    def _():
        gone = out.at[pl.ds(0, (tiles - 1) * height)]
        pltpu.make_async_copy(gone, gone, near_sem).wait()
        if far:
            gone = stage.at[pl.ds(0, far)]
            pltpu.make_async_copy(gone, gone, far_sem).wait()

    pltpu.make_async_copy(out, out, out_sem).wait()


def body(n, tiles, adjusted, fisher):
    models, height, columns = adjusted.shape
    width = columns // n
    share = width // tiles
    flip = shared(height) and tiles % 2 == 0 and share % 8 == 0
    rows = next(r for r in (16, 8, height) if height % r == 0)
    half, chunks = n // 2, height // rows
    count = half * chunks
    bf16 = jnp.bfloat16
    dma = pltpu.SemaphoreType.DMA
    if flip:
        hold = [
            pltpu.VMEM((half, height // LANES + 1, width, LANES), bf16),
            pltpu.VMEM((LANES + LANES // 2, width), bf16),
            pltpu.VMEM((half, LANES // 2, width), bf16),
        ]
        ends = [dma((1 + half,)), dma((2,)), dma((2,)), dma]
    else:
        hold = [pltpu.VMEM((count, tiles, rows, share), bf16), pltpu.VMEM((rows, width), bf16)]
        ends = [dma, dma, dma]
    out = (share, tiles * height) if flip else (tiles * height, share)
    merged = pl.pallas_call(
        functools.partial(flipped if flip else plain, n, tiles, rows, width, share),
        out_shape=pltpu.VMEM(out, bf16),
        in_specs=[pl.BlockSpec(memory_space=pl.ANY)] * 2,
        out_specs=pl.BlockSpec(memory_space=pl.ANY),
        scratch_shapes=[
            pltpu.VMEM((2, count, rows, 2 * width), bf16),
            pltpu.VMEM((2, count, 1, LANES), jnp.float32),
            pltpu.VMEM((2, 2, models, rows, width), bf16),
            pltpu.VMEM((2, 2, models, rows, width), bf16),
            pltpu.VMEM((2, SLOTS, rows, 2 * width), bf16),
            pltpu.VMEM((2, SLOTS, 1, LANES), jnp.float32),
            *hold,
            dma((2, 2, 2)),
            dma((2, SLOTS)),
            dma((2, count)),
            dma((2, SLOTS)),
            dma((2, count)),
            *ends,
        ],
        compiler_params=pltpu.CompilerParams(collective_id=0, has_side_effects=True, vmem_limit_bytes=53 * 1024 * 1024),
    )(adjusted, fisher)
    return merged.T if flip else merged


def solution(mesh):
    return jax.shard_map(
        functools.partial(body, mesh.shape["task"], mesh.shape["tile"]),
        mesh=mesh,
        in_specs=(P("task", "tile", None), P("task", "tile", None)),
        out_specs=P(None, ("task", "tile")),
        check_vma=False,
    )
```
